256 devices in a mesh: dp: 8 (over z), expert: 32 (over y, x, core).
Axes of the slice: x: 4, y: 4, z: 8, core: 2. Of those that a mesh axis runs over, the one named last changes fastest.
Arguments:
- tokens: bfloat16 [65536, 1280], P(('dp', 'expert')), may hold values from -14 to 14
- ln_gain: float32 [1280], replicated, may hold values from 0.25 to 1.75
- router: bfloat16 [1280, 32], replicated, may hold values from -0.3125 to 0.3125
- w_in: bfloat16 [32, 5120, 1280], P('expert', 'dp'), may hold values from -0.15625 to 0.15625
- b_in: bfloat16 [32, 5120], P('expert', 'dp'), may hold values from -3 to 3
- w_out: bfloat16 [32, 5120, 1280], P('expert', 'dp'), may hold values from -0.078125 to 0.078125
- b_out: bfloat16 [32, 1280], P('expert'), may hold values from -3 to 3
- expert_choice: int32 [65536], P(('dp', 'expert')), may hold values from 0 to 31
- modality: int32 [65536], P(('dp', 'expert')), may hold values from 0 to 1, as said below
- slot: int32 [65536], P(('dp', 'expert')), may hold values from -1 to 15, as said below
Outputs:
- moe_out: bfloat16 [65536, 1280], P(('dp', 'expert'))
- aux_losses: float32 [2, 2], replicated
The draws below stay inside these ranges and needn't reach their ends.
Inputs may be any that keep to these rules, and one draw needn't show every extreme that they name: Each source's tokens with one expert and a slot other than -1 have distinct slots, numbered from 0 in token order; one expert has all 16 slots filled in every source. `modality`: every source holds tokens of both modalities.
All inputs are finite; a program needn't handle non-finite values.
Results may differ from the reference program's by a relative error of at most 0.007.
Values may be sent and summed in bfloat16 or wider, within the bound.
A program may use at most 128 MiB of HBM per device.

```python
import jax
import jax.numpy as jnp
from jax import lax

D = 1280
FF = 5120
TOK_DEV = 256
EXPERTS = 32
CAP = 16
TOKENS = 65536


def routing(key):
    base = jax.random.fold_in(key, 7)
    keys = jax.random.split(base, 5)
    blocks = TOKENS // TOK_DEV
    order = jax.random.permutation(keys[0], EXPERTS)
    first = jax.random.randint(keys[1], (blocks, TOK_DEV), 0, EXPERTS)
    second = jax.random.randint(keys[2], (blocks, TOK_DEV), 0, EXPERTS)
    lowest = jnp.minimum(first, second)
    position = jax.vmap(lambda k: jax.random.permutation(k, TOK_DEV))(jax.random.split(keys[3], blocks))
    lowest = jnp.where(position < CAP, 0, lowest)
    chosen = order[lowest].astype(jnp.int32)
    table = (chosen[:, :, None] == jnp.arange(EXPERTS, dtype=jnp.int32)[None, None, :]).astype(jnp.int32)
    before = jnp.cumsum(table, axis=1) - table
    rank = jnp.sum(before * table, axis=-1)
    slots = jnp.where(rank < CAP, rank, -1).astype(jnp.int32)
    kinds = (jax.random.randint(keys[4], (blocks, TOK_DEV), 0, 4) == 0).astype(jnp.int32)
    kinds = jnp.where(position == CAP, 1, kinds)
    kinds = jnp.where(position == CAP + 1, 0, kinds).astype(jnp.int32)
    return (chosen.reshape(TOKENS), kinds.reshape(TOKENS), slots.reshape(TOKENS))


def draw_expert_choice(key, part):
    return routing(key)[0]


def draw_modality(key, part):
    return routing(key)[1]


def draw_slot(key, part):
    return routing(key)[2]


def draw_tokens(key, part):
    blocks = TOKENS // TOK_DEV
    kinds = routing(key)[1].reshape(blocks, TOK_DEV)
    keys = jax.random.split(jax.random.fold_in(key, 11), 2)
    noise = jax.random.normal(keys[0], (blocks, TOK_DEV, D), jnp.float32)
    highest = 3.0
    directions = jnp.clip(jax.random.normal(keys[1], (2, D), jnp.float32), -2.5, 2.5)
    level = highest * jnp.arange(blocks, dtype=jnp.float32) / max(blocks - 1, 1)
    chosen = jnp.where(kinds[:, :, None] == 1, directions[1][None, None, :], directions[0][None, None, :])
    values = jnp.clip(noise, -6.0, 6.0) + level[:, None, None] * chosen
    return jnp.clip(values, -14.0, 14.0).reshape(TOKENS, D).astype(jnp.bfloat16)


def block_scale(rng, shape, cuts, least, high):
    def one(axis_at, shards_of):
        heights = jax.random.uniform(jax.random.fold_in(jax.random.fold_in(rng, 6), axis_at), (shards_of,), jnp.float32, least / len(cuts), high / len(cuts))
        return jnp.repeat(jnp.exp(heights), shape[axis_at] // shards_of).reshape((-1,) + (1,) * (len(shape) - axis_at - 1))

    gain = one(*cuts[0])
    for cut in cuts[1:]:
        gain = gain * one(*cut)
    return gain


def normal_values(rng, shape, deviation, bound, cuts=(), kind=jnp.bfloat16):
    level = block_scale(rng, shape, cuts, -0.22, 0.18) if cuts else 1.0
    drawn = jax.random.normal(rng, shape, jnp.float32) * deviation * level
    return jnp.minimum(jnp.maximum(drawn, -bound), bound).astype(kind)


def setup_inputs(seed: int = 0) -> dict:
    seeds = jax.random.split(jax.random.key(seed), 11)
    tokens = draw_tokens(jax.random.fold_in(seeds[10], 71), 0)
    ln_gain = jnp.clip(1.0 + 0.15 * jax.random.normal(seeds[1], (D,), jnp.float32), 0.25, 1.75)
    router = normal_values(seeds[2], (D, EXPERTS), (D // 4) ** -0.5, 0.3125)
    w_in = normal_values(seeds[3], (EXPERTS, FF, D), D ** -0.5, 0.15625, ((0, 32), (1, 8)))
    b_in = normal_values(seeds[4], (EXPERTS, FF), 0.5, 3.0, ((0, 32), (1, 8)))
    w_out = normal_values(seeds[5], (EXPERTS, FF, D), FF ** -0.5, 0.078125, ((0, 32), (1, 8)))
    b_out = normal_values(seeds[6], (EXPERTS, D), 0.5, 3.0, ((0, 32),))
    expert_choice = draw_expert_choice(jax.random.fold_in(seeds[10], 71), 0)
    modality = draw_modality(jax.random.fold_in(seeds[10], 71), 0)
    slot = draw_slot(jax.random.fold_in(seeds[10], 71), 0)
    return dict(tokens=tokens, ln_gain=ln_gain, router=router, w_in=w_in, b_in=b_in, w_out=w_out, b_out=b_out, expert_choice=expert_choice, modality=modality, slot=slot)


def layer_norm(tokens, ln_gain):
    values = tokens.astype(jnp.float32)
    center = values - lax.optimization_barrier(jnp.mean(values, axis=-1, keepdims=True))
    spread = lax.optimization_barrier(jnp.mean(center * center, axis=-1, keepdims=True))
    return (center * lax.rsqrt(spread + 1e-06) * ln_gain).astype(jnp.bfloat16)

def reference(tokens, ln_gain, router, w_in, b_in, w_out, b_out, expert_choice, modality, slot):
    normed = layer_norm(tokens, ln_gain)
    logits = jnp.dot(normed, router, preferred_element_type=jnp.float32)
    logp = jax.nn.log_softmax(logits, axis=-1)
    probs = jnp.exp(logp)
    gate = jnp.take_along_axis(probs, expert_choice[:, None].astype(jnp.int32), axis=1)[:, 0]
    blocks = TOKENS // TOK_DEV
    source = (jnp.arange(TOKENS, dtype=jnp.int32) // TOK_DEV).astype(jnp.int32)
    place = jnp.where(slot >= 0, slot, CAP).astype(jnp.int32)
    buffer = jnp.zeros((blocks, EXPERTS, CAP + 1, D), jnp.bfloat16)
    buffer = buffer.at[source, expert_choice, place].set(normed)[:, :, :CAP]
    per_expert = jnp.transpose(buffer, (1, 0, 2, 3)).reshape(EXPERTS, blocks * CAP, D)

    def run_expert(items):
        rows, first, first_bias, second, second_bias = items
        pre = lax.dot_general(rows, first, (((1,), (1,)), ((), ())), preferred_element_type=jnp.float32)
        hidden = jax.nn.gelu(pre + first_bias.astype(jnp.float32), approximate=False).astype(jnp.bfloat16)
        result = jnp.dot(hidden, second, preferred_element_type=jnp.float32) + second_bias.astype(jnp.float32)
        return result.astype(jnp.bfloat16)
    outputs = lax.map(run_expert, (per_expert, w_in, b_in, w_out, b_out)).reshape(EXPERTS, blocks, CAP, D)
    fetched = outputs[expert_choice, source, jnp.minimum(place, CAP - 1)]
    kept = (slot >= 0)[:, None]
    moe_out = jnp.where(kept, gate[:, None] * fetched.astype(jnp.float32), 0.0).astype(jnp.bfloat16)
    textual = (modality == 1).astype(jnp.float32)
    select = jnp.stack([1.0 - textual, textual], axis=0)
    entropy = -lax.optimization_barrier(jnp.sum(probs * logp, axis=-1))
    prob_sum = jnp.dot(select, probs, precision=lax.Precision.HIGHEST)
    ent_sum = jnp.dot(select, entropy, precision=lax.Precision.HIGHEST)
    count = lax.optimization_barrier(jnp.sum(select, axis=1))
    pbar = prob_sum / count[:, None]
    aux_losses = jnp.stack([ent_sum / count, lax.optimization_barrier(jnp.sum(pbar * jnp.log(pbar), axis=1))], axis=1)
    return (moe_out, aux_losses)
```

```python
import functools

import jax
import jax.numpy as jnp
from jax import lax
from jax.experimental import pallas as pl
from jax.experimental.pallas import tpu as pltpu
from jax.sharding import Mesh
from jax.sharding import PartitionSpec as P

CAP = 16
DP, EY, EX = "dp", "expert_y", "expert_x"
EXPERT = (EY, EX)
DP_EXPERT = (DP, EY, EX)
MESH = pl.DeviceIdType.MESH
REL = (0, 1, 3, 2)
N = 8


def layer_norm(tokens, ln_gain):
    values = tokens.astype(jnp.float32)
    center = values - jnp.mean(values, axis=-1, keepdims=True)
    spread = jnp.mean(center * center, axis=-1, keepdims=True)
    return (center * lax.rsqrt(spread + 1e-06) * ln_gain).astype(jnp.bfloat16)


def gelu(x):
    return 0.5 * x * (1.0 + lax.erf(x * 0.7071067811865476))


def kernel(
    ny,
    nx,
    buf,
    w_in,
    b_in,
    w_out,
    b_out,
    stats,
    ret,
    tot,
    rows,
    recvm,
    recvp,
    partm,
    partp,
    own,
    ps,
    outb,
    statz,
    statp,
    a_send,
    a_recv,
    gp_recv,
    gm_recv,
    g_send,
    rp_recv,
    rm_recv,
    r_send,
    o_send,
    o_recv,
    s_send,
    s_recv,
):
    rc = nx * CAP
    rb = ny * rc
    z, y, x = lax.axis_index(DP), lax.axis_index(EY), lax.axis_index(EX)
    up, down = lax.rem(z + 1, N), lax.rem(z + N - 1, N)
    expert = y * nx + x

    def at(z_to, y_to, x_to):
        return {DP: z_to, EY: y_to, EX: x_to}

    def send(src, dst, ssem, rsem, to):
        copy = pltpu.make_async_remote_copy(
            src_ref=src, dst_ref=dst, send_sem=ssem, recv_sem=rsem, device_id=to, device_id_type=MESH
        )
        copy.start()

    def arrived(dst, rsem):
        pltpu.make_async_copy(dst, dst, rsem).wait()

    barrier = pltpu.get_barrier_semaphore()

    @pl.loop(1, N)
    def _(k):
        pl.semaphore_signal(barrier, inc=1, device_id=at(lax.rem(z + k, N), y, x), device_id_type=MESH)

    @pl.loop(1, ny * nx)
    def _(k):
        other = lax.rem(expert + k, ny * nx)
        pl.semaphore_signal(
            barrier, inc=1, device_id=at(z, lax.div(other, nx), lax.rem(other, nx)), device_id_type=MESH
        )

    pl.semaphore_wait(barrier, N - 1 + ny * nx - 1)

    mine = pl.ds(pl.multiple_of(x * CAP, CAP), CAP)
    rows[mine, :] = buf[pl.ds(pl.multiple_of(expert * CAP, CAP), CAP), :]
    for c in range(ny):
        y_to = lax.rem(y + ny - REL[c], ny)
        spot = pl.ds(pl.multiple_of(c * rc + x * CAP, CAP), CAP)

        @pl.loop(0 if c else 1, nx)
        def _(k):
            x_to = lax.rem(x + k, nx)
            src = pl.ds(pl.multiple_of((y_to * nx + x_to) * CAP, CAP), CAP)
            send(buf.at[src], rows.at[spot], a_send.at[c], a_recv.at[c], at(z, y_to, x_to))

    statz[0] = stats[...]

    @pl.loop(1, N)
    def _(k):
        send(stats, statz.at[k], s_send.at[0], s_recv.at[0], at(lax.rem(z + k, N), y, x))

    def chunk(d, c):
        return pl.ds(pl.multiple_of(d * rb + c * rc, CAP), rc)

    def gather_up(d, c):
        send(rows.at[chunk(d, c)], rows.at[chunk(d + 1, c)], g_send.at[0], gp_recv.at[d + 1, c], at(up, y, x))

    def gather_down(d, c):
        src = d % N
        send(rows.at[chunk(src, c)], rows.at[chunk(d - 1, c)], g_send.at[1], gm_recv.at[d - 1, c], at(down, y, x))

    def have_up(d, c):
        arrived(rows.at[chunk(d, c)], gp_recv.at[d, c])

    def have_down(d, c):
        arrived(rows.at[chunk(d, c)], gm_recv.at[d, c])

    def ffn(xs):
        pre = lax.dot_general(xs, w_in[...], (((1,), (1,)), ((), ())), preferred_element_type=jnp.float32)
        hidden = gelu(pre + b_in[...]).astype(jnp.bfloat16)
        return jnp.dot(hidden, w_out[...], preferred_element_type=jnp.float32)

    for p in range(2):
        a, b = 2 * p, 2 * p + 1
        for c in (a, b):
            n_in = rc if c else rc - CAP
            arrived(rows.at[pl.ds(c * rc, n_in)], a_recv.at[c])
            gather_up(0, c)
            gather_down(N, c)
        for s in range(1, 4):
            for c in (a, b):
                have_up(s, c)
                if s < 3 or c == a:
                    gather_up(s, c)
                have_down(N - s, c)
                if s < 3 or c == b:
                    gather_down(N - s, c)
        if p == 0:
            have_up(4, a)
            have_down(4, b)
            total = statz[0]
            arrived(statz.at[pl.ds(1, N - 1)], s_recv.at[0])
            for k in range(1, N):
                total = total + statz[k]
            statp[0] = total

            @pl.loop(1, ny * nx)
            def _(k):
                other = lax.rem(expert + k, ny * nx)
                send(
                    statp.at[0],
                    statp.at[k],
                    s_send.at[1],
                    s_recv.at[1],
                    at(z, lax.div(other, nx), lax.rem(other, nx)),
                )

    @pl.loop(0, ny * rc // 256 if ny * rc >= 256 else 1)
    def _(k):
        m = min(256, ny * rc)
        here = pl.ds(pl.multiple_of(k * m, CAP), m)
        own[here, :] = ffn(rows[here, :])

    def finish(c):
        here = pl.ds(c * rc, rc)
        arrived(recvm.at[pl.ds(c * rc, rc)], rm_recv.at[0, c])
        arrived(recvp.at[pl.ds(3 * rb + c * rc, rc)], rp_recv.at[3, c])
        total = own[here, :] + b_out[...]
        total = total + recvm[pl.ds(c * rc, rc), :].astype(jnp.float32)
        total = total + recvp[pl.ds(3 * rb + c * rc, rc), :].astype(jnp.float32)
        outb[here, :] = total.astype(jnp.bfloat16)
        y_to = lax.rem(y + REL[c], ny)
        to = pl.ds(pl.multiple_of(expert * CAP, CAP), CAP)

        @pl.loop(0 if c else 1, nx)
        def _(k):
            x_to = lax.rem(x + k, nx)
            src = pl.ds(pl.multiple_of(c * rc + x_to * CAP, CAP), CAP)
            send(outb.at[src], ret.at[to], o_send.at[0], o_recv.at[0], at(z, y_to, x_to))

        if c == 0:
            ret[to, :] = outb[mine, :]

    @pl.loop(0, 14)
    def _(t):
        p = lax.div(t, 7)
        i = lax.rem(t, 7)
        k = lax.div(i + 1, 2)
        odd = lax.rem(i, 2)
        cm = 2 * p + odd
        cp = 2 * p + 1 - odd

        @pl.when(t == 7)
        def _():
            have_up(4, 2)
            have_down(4, 3)

        sm = chunk(4 - k, cm)
        sp = chunk(4 + k, cp)
        ps[...] = ffn(jnp.concatenate([rows[sm, :], rows[sp, :]], axis=0))
        om = chunk(4 - k, cm)
        mm = pl.ds(pl.multiple_of((3 - k) * rb + cm * rc, CAP), rc)
        pp = pl.ds(pl.multiple_of(k * rb + cp * rc, CAP), rc)

        @pl.when(i < 2)
        def _():
            partm[mm, :] = ps[pl.ds(0, rc), :].astype(jnp.bfloat16)
            partp[pp, :] = ps[pl.ds(rc, rc), :].astype(jnp.bfloat16)

        @pl.when(i >= 2)
        def _():
            got_m = pl.ds(pl.multiple_of((4 - k) * rb + cm * rc, CAP), rc)
            arrived(recvm.at[got_m], rm_recv.at[4 - k, cm])
            partm[mm, :] = (ps[pl.ds(0, rc), :] + recvm[got_m, :].astype(jnp.float32)).astype(jnp.bfloat16)
            got_p = pl.ds(pl.multiple_of((k - 1) * rb + cp * rc, CAP), rc)
            arrived(recvp.at[got_p], rp_recv.at[k - 1, cp])
            partp[pp, :] = (ps[pl.ds(rc, rc), :] + recvp[got_p, :].astype(jnp.float32)).astype(jnp.bfloat16)

        send(partm.at[mm], recvm.at[mm], r_send.at[0], rm_recv.at[3 - k, cm], at(down, y, x))
        send(partp.at[pp], recvp.at[pp], r_send.at[1], rp_recv.at[k, cp], at(up, y, x))

        @pl.when(t == 9)
        def _():
            finish(0)
            finish(1)

    total = statp[0]
    arrived(statp.at[pl.ds(1, ny * nx - 1)], s_recv.at[1])
    for k in range(1, ny * nx):
        total = total + statp[k]
    tot[...] = total
    finish(2)
    finish(3)
    arrived(ret.at[pl.ds(0, ny * rc - CAP)], o_recv.at[0])
    arrived(ret.at[pl.ds(0, ny * rc - CAP)], o_send.at[0])
    for c in range(ny):
        arrived(buf.at[pl.ds(0, rc if c else rc - CAP)], a_send.at[c])
    for k in range(2):
        arrived(rows.at[pl.ds(0, 14 * rc)], g_send.at[k])
        arrived(partm.at[pl.ds(0, 14 * rc)], r_send.at[k])
    arrived(statz.at[pl.ds(1, N - 1)], s_send.at[0])
    arrived(statp.at[pl.ds(1, ny * nx - 1)], s_send.at[1])


def exchange(ny, nx, buf, w_in, b_in, w_out, b_out, stats):
    columns, width = buf.shape
    ff = w_in.shape[0]
    rc = nx * CAP
    vmem = pl.BlockSpec(memory_space=pltpu.VMEM)
    dma = pltpu.SemaphoreType.DMA
    return pl.pallas_call(
        functools.partial(kernel, ny, nx),
        out_shape=(
            jax.ShapeDtypeStruct((columns, width), jnp.bfloat16),
            jax.ShapeDtypeStruct(stats.shape, jnp.float32),
        ),
        in_specs=[vmem] * 6,
        out_specs=(vmem, vmem),
        scratch_shapes=[
            pltpu.VMEM((N * columns, width), jnp.bfloat16),
            pltpu.VMEM((4 * columns, width), jnp.bfloat16),
            pltpu.VMEM((4 * columns, width), jnp.bfloat16),
            pltpu.VMEM((4 * columns, width), jnp.bfloat16),
            pltpu.VMEM((4 * columns, width), jnp.bfloat16),
            pltpu.VMEM((columns, width), jnp.float32),
            pltpu.VMEM((2 * rc, width), jnp.float32),
            pltpu.VMEM((columns, width), jnp.bfloat16),
            pltpu.VMEM((N,) + stats.shape, jnp.float32),
            pltpu.VMEM((ny * nx,) + stats.shape, jnp.float32),
            dma((ny,)),
            dma((ny,)),
            dma((5, ny)),
            dma((8, ny)),
            dma((2,)),
            dma((4, ny)),
            dma((4, ny)),
            dma((2,)),
            dma((1,)),
            dma((1,)),
            dma((2,)),
            dma((2,)),
        ],
        compiler_params=pltpu.CompilerParams(
            collective_id=0, has_side_effects=True, vmem_limit_bytes=60 * 1024 * 1024
        ),
    )(buf, w_in, b_in, w_out, b_out, stats)


def on_device(tokens, ln_gain, router, w_in, b_in, w_out, b_out, expert_choice, modality, slot):
    ny, nx = lax.axis_size(EY), lax.axis_size(EX)
    normed = layer_norm(tokens, ln_gain)
    logits = jnp.dot(normed, router, preferred_element_type=jnp.float32)
    logp = jax.nn.log_softmax(logits, axis=-1)
    probs = jnp.exp(logp)
    experts_all = router.shape[1]
    columns = experts_all * CAP
    picked = expert_choice[:, None] == jnp.arange(experts_all, dtype=jnp.int32)[None, :]
    gate = jnp.sum(jnp.where(picked, probs, 0.0), axis=1)
    target = jnp.where(slot >= 0, expert_choice * CAP + slot, -1)
    table = (target[:, None] == jnp.arange(columns, dtype=jnp.int32)[None, :]).astype(jnp.bfloat16)
    buffer = jnp.einsum("tk,td->kd", table, normed, preferred_element_type=jnp.float32).astype(jnp.bfloat16)

    textual = (modality == 1).astype(jnp.float32)
    select = jnp.stack([1.0 - textual, textual], axis=0)
    entropy = -jnp.sum(probs * logp, axis=-1)
    per_token = jnp.concatenate([probs, entropy[:, None], jnp.ones_like(entropy)[:, None]], axis=1)
    part = jnp.dot(select, per_token, precision=lax.Precision.HIGHEST)
    stats = jnp.pad(part, ((0, 6), (0, 128 - part.shape[1])))

    returned, total = exchange(
        ny,
        nx,
        buffer,
        w_in[0],
        b_in.astype(jnp.float32),
        w_out[0],
        b_out.astype(jnp.float32),
        stats,
    )
    fetched = jnp.dot(table, returned, preferred_element_type=jnp.float32)
    moe_out = (gate[:, None] * fetched).astype(jnp.bfloat16)
    prob_sum, ent_sum, count = total[:2, :experts_all], total[:2, experts_all], total[:2, experts_all + 1]
    pbar = prob_sum / count[:, None]
    aux_losses = jnp.stack([ent_sum / count, jnp.sum(pbar * jnp.log(pbar), axis=1)], axis=1)
    return (moe_out, aux_losses)


def solution(mesh):
    finer = Mesh(mesh.devices.reshape(mesh.shape["dp"], 4, 8), (DP, EY, EX))
    return jax.shard_map(
        on_device,
        mesh=finer,
        in_specs=(
            P(DP_EXPERT, None),
            P(),
            P(),
            P(EXPERT, DP, None),
            P(EXPERT, DP),
            P(EXPERT, DP, None),
            P(EXPERT, None),
            P(DP_EXPERT),
            P(DP_EXPERT),
            P(DP_EXPERT),
        ),
        out_specs=(P(DP_EXPERT, None), P()),
        check_vma=False,
    )
```
